256 devices in a mesh: doc: 2 (over z), seq: 16 (over y, core), head: 8 (over x).
Axes of the slice: x: 8, y: 8, z: 2, core: 2. Of those that a mesh axis runs over, the one named last changes fastest.
The devices are a block of a 8x8x16 slice.
Arguments:
- length: int32 [2], P('doc'), parts along dimension 0, may hold values from 3968 to 4096
- residual: bfloat16 [8192, 4096], P(('doc', 'seq'), 'head'), parts along dimension 0, may hold values from -6 to 6
- ssm_input: bfloat16 [8192, 4096], P(('doc', 'seq'), 'head'), parts along dimension 0, may hold values from -6 to 6
- state_in: bfloat16 [8192, 128], P(('doc', 'seq')), parts along dimension 0, may hold values from -6 to 6
- state_out: bfloat16 [8192, 128], P(('doc', 'seq')), parts along dimension 0, may hold values from -0.5 to 0.5
- step_raw: float32 [128, 4096], P(('doc', 'head'), 'seq'), parts along dimension 0, may hold values from -5 to 2
- decay_rate: float32 [64], P('head'), may hold values from 0 to 1, as said below
- ssm_gain: float32 [4096], P('head'), may hold values from 0.1 to 1.9
- out_weight: bfloat16 [4096, 4096], P('head'), may hold values from -0.09375 to 0.09375
- norm_gain: float32 [4096], replicated, may hold values from 0.1 to 1.9
- query_weight: bfloat16 [4096, 4096], P(None, 'head'), may hold values from -2 to 2
- key_weight: bfloat16 [4096, 1024], P(None, 'head'), may hold values from -3 to 3
- value_weight: bfloat16 [4096, 1024], P(None, 'head'), may hold values from -0.09375 to 0.09375
Outputs:
- layer_out: bfloat16 [8192, 4096], P(('doc', 'seq'), 'head'), parts along dimension 0
- head_out: bfloat16 [8192, 4096], P(('doc', 'seq'), 'head'), parts along dimension 0
The draws below stay inside these ranges and needn't reach their ends.
There are 2 independent parts, one for each index of `doc`. The reference program is written for one: setup_inputs(seed, part) draws one part's arguments, and reference() takes and returns one part's arrays. A program takes and returns all parts, laid end to end along the dimension named above; an argument that names none is the same for every part. Nothing has to cross between parts.
Inputs may be any that keep to these rules, and one draw needn't show every extreme that they name: The document fills positions 0 to length - 1 of the 4096; later positions are padding. `decay_rate`: positive.
All inputs are finite; a program needn't handle non-finite values.
Results may differ from the reference program's by a relative error of at most 0.028.
The reference program's roundings to bfloat16 on the way count: a program that leaves them out, or rounds other values in their place, can miss the bound.
Values may be sent and summed in bfloat16 or wider, within the bound.
A program may use at most 64 MiB of HBM per device.

```python
import jax
import jax.numpy as jnp
from jax import lax

D = 4096
SSM_HEADS = 64
SSM_HDIM = 64
STATE = 128
Q_HEADS = 32
KV_HEADS = 8
HEAD_DIM = 128
TOK_DEV = 256
INNER = 4096
TOKENS = 4096


def draw_step_raw(key, part):
    blocks = TOKENS // TOK_DEV
    base = jax.random.uniform(jax.random.fold_in(key, 31), (SSM_HEADS, blocks, TOK_DEV), jnp.float32, -3.5, 1.0)
    offset = jax.random.uniform(jax.random.fold_in(key, 32), (SSM_HEADS, blocks, 1), jnp.float32, -1.5, 1.0)
    return (base + offset).reshape(SSM_HEADS, TOKENS)


def draw_decay_rate(key, part):
    order = jax.random.permutation(jax.random.fold_in(key, 21), SSM_HEADS)
    slow = order < SSM_HEADS // 2
    spread = jax.random.uniform(jax.random.fold_in(key, 22), (SSM_HEADS,), jnp.float32)
    slow_rate = jnp.exp(jnp.log(0.25 / TOKENS) + spread * jnp.log(12.0))
    fast_rate = jnp.exp(jnp.log(0.05) + spread * jnp.log(20.0))
    return jnp.where(slow, slow_rate, fast_rate)


def query_key_pair(key):
    scale = 1.6 * D ** (-0.5)
    query_part = jnp.clip(jax.random.normal(jax.random.fold_in(key, 11), (D, Q_HEADS * HEAD_DIM), jnp.float32), -6.0, 6.0) * scale
    key_part = jnp.clip(jax.random.normal(jax.random.fold_in(key, 12), (D, KV_HEADS * HEAD_DIM), jnp.float32), -6.0, 6.0) * scale
    return (query_part, key_part)


def draw_query_weight(key, part):
    return query_key_pair(key)[0].astype(jnp.bfloat16)


def draw_key_weight(key, part):
    return query_key_pair(key)[1].astype(jnp.bfloat16)


def levels(stream_key, extent, split, smallest, top_value):
    gain, own = 1.0, jax.random.fold_in(stream_key, 6)
    for dim, blocks in split:
        heights = jnp.exp(jax.random.uniform(jax.random.fold_in(own, dim), (blocks,), jnp.float32, smallest / len(split), top_value / len(split)))
        gain = gain * jnp.repeat(heights, extent[dim] // blocks).reshape([-1 if axis == dim else 1 for axis in range(len(extent))])
    return gain


def centred(rng, extent, scale, reach, shards=(), kind=jnp.bfloat16):
    drawn = scale * jax.random.normal(rng, extent, jnp.float32)
    if shards:
        drawn = drawn * levels(rng, extent, shards, -0.22, 0.18)
    return jnp.clip(drawn, -reach, reach).astype(kind)


def setup_inputs(seed: int = 0, part: int = 0) -> dict:
    key_list = jax.random.split(jax.random.key(seed), 14)
    part_keys = jax.random.split(jax.random.fold_in(key_list[13], part), 14)
    length = jax.random.randint(part_keys[0], (1,), TOKENS - TOK_DEV // 2, TOKENS + 1).astype(jnp.int32)
    residual = centred(part_keys[1], (TOKENS, D), 1.0, 6.0, ((0, 16), (1, 8)))
    ssm_input = centred(part_keys[2], (TOKENS, INNER), 1.0, 6.0, ((0, 16), (1, 8)))
    state_in = centred(part_keys[3], (TOKENS, STATE), 1.0, 6.0, ((0, 16),))
    state_out = centred(part_keys[4], (TOKENS, STATE), STATE ** -0.5, 0.5, ((0, 16),))
    step_raw = draw_step_raw(jax.random.fold_in(jax.random.fold_in(key_list[13], part), 71), part)
    decay_rate = draw_decay_rate(jax.random.fold_in(key_list[13], 71), part)
    ssm_gain = jnp.clip(1.0 + 0.18 * jax.random.normal(key_list[7], (INNER,), jnp.float32), 0.1, 1.9)
    out_weight = centred(key_list[8], (INNER, D), INNER ** -0.5, 0.09375, ((0, 8),))
    norm_gain = jnp.clip(1.0 + 0.18 * jax.random.normal(key_list[9], (D,), jnp.float32), 0.1, 1.9)
    query_weight = draw_query_weight(jax.random.fold_in(key_list[13], 71), part)
    key_weight = draw_key_weight(jax.random.fold_in(key_list[13], 71), part)
    value_weight = centred(key_list[12], (D, KV_HEADS * HEAD_DIM), D ** -0.5, 0.09375, ((1, 8),))
    return dict(length=length, residual=residual, ssm_input=ssm_input, state_in=state_in, state_out=state_out, step_raw=step_raw, decay_rate=decay_rate, ssm_gain=ssm_gain, out_weight=out_weight, norm_gain=norm_gain, query_weight=query_weight, key_weight=key_weight, value_weight=value_weight)


EPSILON = 1e-05
NEG_BIG = -1e+30
HIGHEST = lax.Precision.HIGHEST

def ssd_blocks(ssm_input, state_in, state_out, delta, decay_rate):
    blocks = TOKENS // TOK_DEV
    inputs = ssm_input.astype(jnp.float32).reshape(blocks, TOK_DEV, SSM_HEADS, SSM_HDIM)
    enter = state_in.reshape(blocks, TOK_DEV, STATE)
    leave = state_out.reshape(blocks, TOK_DEV, STATE)
    steps = delta.reshape(SSM_HEADS, blocks, TOK_DEV).transpose(1, 0, 2)
    causal = jnp.arange(TOK_DEV)[:, None] >= jnp.arange(TOK_DEV)[None, :]

    def advance(carried, inputs_now):
        block_in, enter_now, leave_now, step_now = inputs_now
        cumlog = jnp.cumsum(-decay_rate[:, None] * step_now, axis=1)
        inner = jnp.dot(leave_now, enter_now.T, preferred_element_type=jnp.float32)
        spread = cumlog[:, :, None] - cumlog[:, None, :]
        mixing = jnp.where(causal[None], jnp.exp(jnp.where(causal[None], spread, 0.0)), 0.0) * inner[None] * step_now[:, None, :]
        within = jnp.einsum('hts,shp->thp', mixing, block_in, precision=HIGHEST)
        carried_out = jnp.einsum('hpn,tn->thp', carried, leave_now.astype(jnp.float32), precision=HIGHEST)
        output = within + jnp.exp(cumlog).T[:, :, None] * carried_out
        tail = jnp.exp(cumlog[:, -1:] - cumlog) * step_now
        fresh = jnp.einsum('hs,shp,sn->hpn', tail, block_in, enter_now.astype(jnp.float32), precision=HIGHEST)
        following = jnp.exp(cumlog[:, -1])[:, None, None] * carried + fresh
        return (following, output)
    start = jnp.zeros((SSM_HEADS, SSM_HDIM, STATE), jnp.float32)
    unused, outputs = lax.scan(advance, start, (inputs, enter, leave, steps))
    return outputs.reshape(TOKENS, SSM_HEADS, SSM_HDIM)

def reference(length, residual, ssm_input, state_in, state_out, step_raw, decay_rate, ssm_gain, out_weight, norm_gain, query_weight, key_weight, value_weight):
    positions = jnp.arange(TOKENS, dtype=jnp.int32)
    live_rows = positions < length[0]
    live = live_rows.astype(jnp.float32)
    delta = live[None, :] * jax.nn.softplus(step_raw)
    ssm_out = ssd_blocks(ssm_input, state_in, state_out, delta, decay_rate) * live[:, None, None]
    mean_square = lax.optimization_barrier(jnp.mean(ssm_out * ssm_out, axis=2, keepdims=True))
    normed = (ssm_out * lax.rsqrt(mean_square + EPSILON) * ssm_gain.reshape(SSM_HEADS, SSM_HDIM)).astype(jnp.bfloat16)
    normed = normed.reshape(TOKENS, SSM_HEADS * SSM_HDIM)
    projected = jnp.dot(normed, out_weight, preferred_element_type=jnp.float32)
    layer_out = (residual.astype(jnp.float32) + projected).astype(jnp.bfloat16)
    widened = layer_out.astype(jnp.float32)
    attn_in = (widened * lax.rsqrt(lax.optimization_barrier(jnp.mean(widened * widened, axis=1, keepdims=True)) + EPSILON) * norm_gain).astype(jnp.bfloat16)
    queries = jnp.dot(attn_in, query_weight, preferred_element_type=jnp.float32).astype(jnp.bfloat16)
    keys = jnp.dot(attn_in, key_weight, preferred_element_type=jnp.float32).astype(jnp.bfloat16)
    values = jnp.dot(attn_in, value_weight, preferred_element_type=jnp.float32).astype(jnp.bfloat16)
    group_size = Q_HEADS // KV_HEADS
    query_heads = queries.reshape(TOKENS, Q_HEADS, HEAD_DIM).transpose(1, 0, 2)
    key_heads = jnp.repeat(keys.reshape(TOKENS, KV_HEADS, HEAD_DIM).transpose(1, 0, 2), group_size, axis=0)
    value_heads = jnp.repeat(values.reshape(TOKENS, KV_HEADS, HEAD_DIM).transpose(1, 0, 2), group_size, axis=0)
    allowed = (positions[None, :] <= positions[:, None]) & live_rows[None, :]

    def one_head(operands):
        query_now, key_now, value_now = operands
        scores = jnp.dot(query_now, key_now.T, preferred_element_type=jnp.float32) * HEAD_DIM ** (-0.5)
        masked = jnp.where(allowed, scores, NEG_BIG)
        best = lax.optimization_barrier(jnp.max(masked, axis=1, keepdims=True))
        weights = jnp.where(allowed, jnp.exp(masked - best), 0.0)
        total = lax.optimization_barrier(jnp.sum(weights, axis=1, keepdims=True))
        mixed = jnp.dot(weights.astype(jnp.bfloat16), value_now, preferred_element_type=jnp.float32)
        return mixed / jnp.where(live_rows[:, None], total, 1.0) * live[:, None]
    heads = lax.map(one_head, (query_heads, key_heads, value_heads))
    head_out = heads.transpose(1, 0, 2).reshape(TOKENS, Q_HEADS * HEAD_DIM).astype(jnp.bfloat16)
    return (layer_out, head_out)
```

```python
import functools

import jax
import jax.numpy as jnp
from jax import lax
from jax.experimental import pallas as pl
from jax.experimental.pallas import tpu as pltpu
from jax.sharding import Mesh
from jax.sharding import PartitionSpec as P

HEAD_DIM = 128
EPSILON = 1e-05
DOC_SEQ = ("doc", "seq_0", "seq_1")
SEQ = ("seq_0", "seq_1")
MESH = pl.DeviceIdType.MESH
VMEM = pl.BlockSpec(memory_space=pltpu.VMEM)
SMEM = pl.BlockSpec(memory_space=pltpu.SMEM)
F32 = jnp.float32
BF16 = jnp.bfloat16

SUB = 4


def contract(a, b, dims):
    return lax.dot_general(a, b, (dims, ((), ())), preferred_element_type=F32)


def two_terms(x):
    high = x.astype(BF16)
    return high, (x - high.astype(F32)).astype(BF16)


def seq_peer(index):
    return {"seq_0": index // 2, "seq_1": index % 2}


def ssm_kernel(
    n,
    length_ref,
    x_ref,
    b_ref,
    c_ref,
    step_ref,
    decay_ref,
    gain_ref,
    normed_ref,
    stage,
    arrived,
    prefix,
    incoming,
    within,
    out_sems,
    in_sems,
    back_sems,
    home_sems,
):
    me = lax.axis_index("seq_0") * 2 + lax.axis_index("seq_1")
    rows, width = x_ref.shape
    heads = step_ref.shape[0]
    head_width = width // heads
    piece = width // n
    per_head = head_width // piece

    barrier = pltpu.get_barrier_semaphore()
    for o in range(1, n):
        pl.semaphore_signal(
            barrier, inc=1, device_id=seq_peer(lax.rem(me + o, n)), device_id_type=MESH
        )

    limit = length_ref[0]
    along = lax.broadcasted_iota(jnp.int32, (1, rows), 1) + me * rows
    live_row = (along < limit).astype(F32)
    down = lax.broadcasted_iota(jnp.int32, (rows, 1), 0) + me * rows
    live_col = (down < limit).astype(F32)
    raw = step_ref[...]
    delta = live_row * (jnp.maximum(raw, 0.0) + jnp.log1p(jnp.exp(-jnp.abs(raw))))
    t_of = lax.broadcasted_iota(jnp.int32, (rows, rows), 0)
    s_of = lax.broadcasted_iota(jnp.int32, (rows, rows), 1)
    causal = t_of >= s_of
    upper = (t_of <= s_of).astype(F32)
    cumlog = lax.dot_general(
        -decay_ref[...] * delta,
        upper,
        (((1,), (0,)), ((), ())),
        precision=lax.Precision.HIGHEST,
        preferred_element_type=F32,
    )
    last = cumlog[:, rows - 1 : rows]
    tail_t = jnp.transpose(jnp.exp(last - cumlog) * delta)
    cumlog_t = jnp.transpose(cumlog)
    block_decay = jnp.broadcast_to(jnp.exp(last), (heads, 128))
    lanes = lax.broadcasted_iota(jnp.int32, (rows, 128), 1)
    first = lanes < head_width

    for pair in range(width // 128):
        a, b = 2 * pair, 2 * pair + 1
        scale = jnp.where(first, tail_t[:, a : a + 1], tail_t[:, b : b + 1])
        high, low = two_terms(x_ref[:, 128 * pair : 128 * (pair + 1)].astype(F32) * scale)
        state = contract(high, b_ref[...], ((0,), (0,))) + contract(low, b_ref[...], ((0,), (0,)))
        for q in range(128 // piece):
            j = pair * (128 // piece) + q
            stage[j, 0:piece] = state[q * piece : (q + 1) * piece]
            h = j // per_head
            stage[j, piece : piece + 8] = jnp.broadcast_to(block_decay[h : h + 1], (8, 128))

    pl.semaphore_wait(barrier, n - 1)

    def out_copy(o):
        peer = lax.rem(me + o, n)
        return pltpu.make_async_remote_copy(
            src_ref=stage.at[peer],
            dst_ref=arrived.at[me],
            send_sem=out_sems.at[o],
            recv_sem=in_sems.at[o],
            device_id=seq_peer(peer),
            device_id_type=MESH,
        )

    order = sorted(range(1, n), key=lambda o: -min(o, n - o))
    for o in order:
        out_copy(o).start()
    arrived[me] = stage[me]

    inner = contract(c_ref[...], b_ref[...], ((1,), (1,)))
    for pair in range(width // 128):
        values = x_ref[:, 128 * pair : 128 * (pair + 1)]
        parts = []
        for h in (2 * pair, 2 * pair + 1):
            spread = cumlog_t[:, h : h + 1] - cumlog[h : h + 1, :]
            mixing = jnp.exp(jnp.where(causal, spread, -1e30)) * inner * delta[h : h + 1, :]
            high, low = two_terms(mixing)
            parts.append(
                contract(high, values, ((1,), (0,))) + contract(low, values, ((1,), (0,)))
            )
        within[:, 128 * pair : 128 * (pair + 1)] = jnp.where(first, parts[0], parts[1])

    for o in order:
        out_copy(o).wait_recv()
    carry = jnp.zeros((piece, 128), F32)
    for i in range(n):
        prefix[i] = carry
        carry = arrived[i, piece : piece + 1] * carry + arrived[i, 0:piece]

    def home_copy(o):
        peer = lax.rem(me + o, n)
        return pltpu.make_async_remote_copy(
            src_ref=prefix.at[peer],
            dst_ref=incoming.at[me],
            send_sem=back_sems.at[o],
            recv_sem=home_sems.at[o],
            device_id=seq_peer(peer),
            device_id_type=MESH,
        )

    for o in order:
        home_copy(o).start()
    incoming[me] = prefix[me]
    for o in order:
        home_copy(o).wait_recv()

    group = (
        lax.broadcasted_iota(jnp.int32, (128, 128), 0) // head_width
        == lax.broadcasted_iota(jnp.int32, (128, 128), 1) // head_width
    ).astype(BF16)
    grown = jnp.exp(cumlog_t)
    for pair in range(width // 128):
        a, b = 2 * pair, 2 * pair + 1
        count = 128 // piece
        state = incoming[pair * count : (pair + 1) * count].reshape(128, 128)
        high, low = two_terms(state)
        carried = contract(c_ref[...], high, ((1,), (1,))) + contract(
            c_ref[...], low, ((1,), (1,))
        )
        scale = jnp.where(first, grown[:, a : a + 1], grown[:, b : b + 1])
        y = (within[:, 128 * pair : 128 * (pair + 1)] + scale * carried) * live_col
        high, low = two_terms(y * y)
        mean = (contract(high, group, ((1,), (0,))) + contract(low, group, ((1,), (0,)))) * (
            1.0 / head_width
        )
        cols = slice(128 * pair, 128 * (pair + 1))
        normed_ref[:, cols] = (y * lax.rsqrt(mean + EPSILON) * gain_ref[:, cols]).astype(BF16)

    for o in order:
        out_copy(o).wait_send()
        home_copy(o).wait_send()


def ssm_layer(length, ssm_input, state_in, state_out, step_raw, decay_rate, ssm_gain):
    rows, width = ssm_input.shape
    n = lax.axis_size(SEQ)
    piece = width // n
    return pl.pallas_call(
        functools.partial(ssm_kernel, n),
        out_shape=jax.ShapeDtypeStruct((rows, width), BF16),
        in_specs=[SMEM] + [VMEM] * 6,
        out_specs=VMEM,
        scratch_shapes=[
            pltpu.VMEM((n, piece + 8, 128), F32),
            pltpu.VMEM((n, piece + 8, 128), F32),
            pltpu.VMEM((n, piece, 128), F32),
            pltpu.VMEM((n, piece, 128), F32),
            pltpu.VMEM((rows, width), F32),
            pltpu.SemaphoreType.DMA((n,)),
            pltpu.SemaphoreType.DMA((n,)),
            pltpu.SemaphoreType.DMA((n,)),
            pltpu.SemaphoreType.DMA((n,)),
        ],
        compiler_params=pltpu.CompilerParams(collective_id=0, has_side_effects=True),
        name="ssm_layer",
    )(
        length,
        ssm_input,
        state_in,
        state_out,
        step_raw,
        decay_rate.reshape(-1, 1),
        ssm_gain.reshape(1, -1),
    )


def depth(direction, s, n):
    long_way = (s < SUB // 2) == (direction == 0)
    return n // 2 if long_way else n - 1 - n // 2


def project_kernel(
    n,
    normed_ref,
    weight_ref,
    residual_ref,
    layer_ref,
    full_ref,
    outgoing,
    arrived,
    sum_send,
    sum_recv,
    all_send,
    all_recv,
):
    me = lax.axis_index("head")
    rows = normed_ref.shape[0]
    width = residual_ref.shape[1]
    block = rows // SUB
    half = rows // 2
    neighbour = (lax.rem(me + n - 1, n), lax.rem(me + 1, n))

    barrier = pltpu.get_barrier_semaphore()
    for d in (0, 1):
        pl.semaphore_signal(
            barrier, inc=1, device_id={"head": neighbour[d]}, device_id_type=MESH
        )
    pl.semaphore_wait(barrier, 2)

    def away(d, steps):
        return lax.rem(me + (n - steps if d == 0 else steps), n)

    def partial(j, side):
        cols = pl.ds(pl.multiple_of(j * width, width), width)
        return contract(
            normed_ref[side * half : (side + 1) * half], weight_ref[:, cols], ((1,), (0,))
        )

    def sum_copy(d, level, s):
        return pltpu.make_async_remote_copy(
            src_ref=outgoing.at[d, level, s],
            dst_ref=arrived.at[d, level, s],
            send_sem=sum_send.at[d, level, s],
            recv_sem=sum_recv.at[d, level, s],
            device_id={"head": neighbour[d]},
            device_id_type=MESH,
        )

    def all_copy(d, level, s):
        owner = away(1 - d, level)
        at = (owner, pl.ds(s * block, block))
        return pltpu.make_async_remote_copy(
            src_ref=full_ref.at[at],
            dst_ref=full_ref.at[at],
            send_sem=all_send.at[d, level, s],
            recv_sem=all_recv.at[d, level, s],
            device_id={"head": neighbour[d]},
            device_id_type=MESH,
        )

    most = n // 2
    for level in range(most):
        for side in (0, 1):
            for d in (0, 1):
                hops = depth(d, side * (SUB // 2), n)
                if level >= hops:
                    continue
                product = partial(away(d, hops - level), side)
                for k in range(SUB // 2):
                    s = side * (SUB // 2) + k
                    value = product[k * block : (k + 1) * block]
                    if level > 0:
                        sum_copy(d, level - 1, s).wait_recv()
                        value = value + arrived[d, level - 1, s].astype(F32)
                    outgoing[d, level, s] = value.astype(BF16)
                    sum_copy(d, level, s).start()

    for side in (0, 1):
        product = partial(me, side)
        for k in range(SUB // 2):
            s = side * (SUB // 2) + k
            here = slice(s * block, (s + 1) * block)
            value = residual_ref[here].astype(F32) + product[k * block : (k + 1) * block]
            for d in (0, 1):
                last = depth(d, s, n) - 1
                sum_copy(d, last, s).wait_recv()
                value = value + arrived[d, last, s].astype(F32)
            value = value.astype(BF16)
            layer_ref[here] = value
            full_ref[me, here] = value
            for d in (0, 1):
                all_copy(d, 0, s).start()

    for level in range(1, most):
        for s in range(SUB):
            for d in (0, 1):
                if level < depth(d, s, n):
                    all_copy(d, level - 1, s).wait_recv()
                    all_copy(d, level, s).start()
    for s in range(SUB):
        for d in (0, 1):
            all_copy(d, depth(d, s, n) - 1, s).wait_recv()
    for s in range(SUB):
        for d in (0, 1):
            for level in range(depth(d, s, n)):
                sum_copy(d, level, s).wait_send()
                all_copy(d, level, s).wait_send()


def project(normed, out_weight, residual):
    rows, width = residual.shape
    n = lax.axis_size("head")
    slots = (2, n // 2, SUB)
    return pl.pallas_call(
        functools.partial(project_kernel, n),
        out_shape=(
            jax.ShapeDtypeStruct((rows, width), BF16),
            jax.ShapeDtypeStruct((n, rows, width), BF16),
        ),
        in_specs=[VMEM] * 3,
        out_specs=(VMEM, VMEM),
        scratch_shapes=[
            pltpu.VMEM((*slots, rows // SUB, width), BF16),
            pltpu.VMEM((*slots, rows // SUB, width), BF16),
            pltpu.SemaphoreType.DMA(slots),
            pltpu.SemaphoreType.DMA(slots),
            pltpu.SemaphoreType.DMA(slots),
            pltpu.SemaphoreType.DMA(slots),
        ],
        compiler_params=pltpu.CompilerParams(
            collective_id=1, has_side_effects=True, vmem_limit_bytes=40 << 20
        ),
        name="project",
    )(normed, out_weight, residual)


def attend_kernel(
    n,
    length_ref,
    full_ref,
    gain_ref,
    wq_ref,
    wk_ref,
    wv_ref,
    out_ref,
    attn_in,
    queries,
    kv,
    best,
    total,
    accum,
    ring_send,
    ring_recv,
    twin_send,
    twin_recv,
):
    y = lax.axis_index("seq_0")
    core = lax.axis_index("seq_1")
    me = y * 2 + core
    chunks, rows, width = full_ref.shape
    heads = width // HEAD_DIM
    neighbour = (lax.rem(y + n - 1, n), lax.rem(y + 1, n))

    barrier = pltpu.get_barrier_semaphore()
    for d in (0, 1):
        pl.semaphore_signal(
            barrier, inc=1, device_id={"seq_0": neighbour[d]}, device_id_type=MESH
        )
    pl.semaphore_signal(barrier, inc=1, device_id={"seq_1": 1 - core}, device_id_type=MESH)

    squares = jnp.zeros((rows, 1), F32)
    for j in range(chunks):
        wide = full_ref[j].astype(F32)
        squares = squares + jnp.sum(wide * wide, axis=1, keepdims=True)
    inverse = lax.rsqrt(squares * (1.0 / (chunks * width)) + EPSILON)
    keys = jnp.zeros((rows, HEAD_DIM), F32)
    values = jnp.zeros((rows, HEAD_DIM), F32)
    for j in range(chunks):
        wide = full_ref[j].astype(F32) * inverse * gain_ref[j : j + 1]
        scaled = wide.astype(BF16)
        attn_in[j] = scaled
        down = slice(j * width, (j + 1) * width)
        keys = keys + contract(scaled, wk_ref[down], ((1,), (0,)))
        values = values + contract(scaled, wv_ref[down], ((1,), (0,)))
    kv[0, me] = keys.astype(BF16)
    kv[1, me] = values.astype(BF16)

    def hops(d, kind):
        long_way = (kind == 0) == (d == 1)
        return n // 2 if long_way else n - 1 - n // 2

    def owner_chip(d, level):
        return lax.rem(y + (level if d == 0 else n - level), n)

    def ring_copy(d, level, kind):
        at = (kind, owner_chip(d, level) * 2 + core)
        return pltpu.make_async_remote_copy(
            src_ref=kv.at[at],
            dst_ref=kv.at[at],
            send_sem=ring_send.at[d, level, kind],
            recv_sem=ring_recv.at[d, level, kind],
            device_id={"seq_0": neighbour[d]},
            device_id_type=MESH,
        )

    def twin_copy(d, level, kind, mine=True):
        chip = y if level < 0 else owner_chip(d, level + 1)
        at = (kind, chip * 2 + (core if mine else 1 - core))
        return pltpu.make_async_remote_copy(
            src_ref=kv.at[at],
            dst_ref=kv.at[at],
            send_sem=twin_send.at[d, level + 1, kind],
            recv_sem=twin_recv.at[d, level + 1, kind],
            device_id={"seq_1": 1 - core},
            device_id_type=MESH,
        )

    pl.semaphore_wait(barrier, 3)
    for kind in (0, 1):
        for d in (1, 0):
            ring_copy(d, 0, kind).start()
    for kind in (0, 1):
        twin_copy(0, -1, kind).start()

    product = jnp.zeros((rows, width), F32)
    for j in range(chunks):
        down = slice(j * width, (j + 1) * width)
        product = product + contract(attn_in[j], wq_ref[down], ((1,), (0,)))
    queries[...] = product.astype(BF16)

    scale = HEAD_DIM**-0.5 * 1.4426950408889634
    t_of = lax.broadcasted_iota(jnp.int32, (rows, rows), 0)
    s_of = lax.broadcasted_iota(jnp.int32, (rows, rows), 1)
    causal = t_of >= s_of
    for h in range(heads):
        cols = slice(h * HEAD_DIM, (h + 1) * HEAD_DIM)
        scores = contract(queries[:, cols], kv[0, me], ((1,), (1,))) * scale
        scores = jnp.where(causal, scores, -1e30)
        top = jnp.max(scores, axis=1, keepdims=True)
        weights = jnp.exp2(scores - top)
        best[h] = jnp.broadcast_to(top, (rows, HEAD_DIM))
        total[h] = jnp.broadcast_to(jnp.sum(weights, axis=1, keepdims=True), (rows, HEAD_DIM))
        accum[h] = contract(weights.astype(BF16), kv[1, me], ((1,), (0,)))

    def fold(key_block, value_block):
        for h in range(heads):
            cols = slice(h * HEAD_DIM, (h + 1) * HEAD_DIM)
            scores = contract(queries[:, cols], key_block, ((1,), (1,))) * scale
            old = best[h][:, 0:1]
            top = jnp.maximum(old, jnp.max(scores, axis=1, keepdims=True))
            weights = jnp.exp2(scores - top)
            shrink = jnp.exp2(old - top)
            best[h] = jnp.broadcast_to(top, (rows, HEAD_DIM))
            total[h] = total[h] * shrink + jnp.sum(weights, axis=1, keepdims=True)
            accum[h] = accum[h] * shrink + contract(
                weights.astype(BF16), value_block, ((1,), (0,))
            )

    def chip_block(kind, chip):
        return kv[kind, pl.ds(chip * 2, 2)].reshape(2 * rows, HEAD_DIM)

    for kind in (0, 1):
        twin_copy(0, -1, kind, mine=False).wait_recv()

    @pl.when(core == 1)
    def _():
        fold(kv[0, y * 2], kv[1, y * 2])

    def forward(d, level):
        for kind in (0, 1):
            if level < hops(d, kind):
                ring_copy(d, level, kind).wait_recv()
                if level + 1 < hops(d, kind):
                    ring_copy(d, level + 1, kind).start()
                twin_copy(d, level, kind).start()

    def both(d, level):
        return all(level < hops(d, kind) for kind in (0, 1))

    for level in range(n // 2):
        for d in (1, 0):
            forward(d, level)
        for d in (1, 0):
            for kind in (0, 1):
                if level < hops(d, kind):
                    twin_copy(d, level, kind, mine=False).wait_recv()
        for d in (1, 0):
            if both(d, level) or (level < hops(1, 0) and d == 1):
                chip = owner_chip(d, level + 1)

                @pl.when(chip < y)
                def _():
                    fold(chip_block(0, chip), chip_block(1, chip))

    live = (
        lax.broadcasted_iota(jnp.int32, (rows, 1), 0) + me * rows < length_ref[0]
    ).astype(F32)
    for h in range(heads):
        cols = slice(h * HEAD_DIM, (h + 1) * HEAD_DIM)
        safe = jnp.where(live > 0.0, total[h], 1.0)
        out_ref[:, cols] = (accum[h] / safe * live).astype(BF16)

    for kind in (0, 1):
        twin_copy(0, -1, kind).wait_send()
        for d in (0, 1):
            for level in range(hops(d, kind)):
                ring_copy(d, level, kind).wait_send()
                twin_copy(d, level, kind).wait_send()


def attend(length, full, norm_gain, query_weight, key_weight, value_weight):
    chunks, rows, width = full.shape
    n = lax.axis_size("seq_0")
    heads = width // HEAD_DIM
    ring = (2, n // 2, 2)
    twin = (2, n // 2 + 1, 2)
    return pl.pallas_call(
        functools.partial(attend_kernel, n),
        out_shape=jax.ShapeDtypeStruct((rows, width), BF16),
        in_specs=[SMEM] + [VMEM] * 5,
        out_specs=VMEM,
        scratch_shapes=[
            pltpu.VMEM((chunks, rows, width), BF16),
            pltpu.VMEM((rows, width), BF16),
            pltpu.VMEM((2, 2 * n, rows, HEAD_DIM), BF16),
            pltpu.VMEM((heads, rows, HEAD_DIM), F32),
            pltpu.VMEM((heads, rows, HEAD_DIM), F32),
            pltpu.VMEM((heads, rows, HEAD_DIM), F32),
            pltpu.SemaphoreType.DMA(ring),
            pltpu.SemaphoreType.DMA(ring),
            pltpu.SemaphoreType.DMA(twin),
            pltpu.SemaphoreType.DMA(twin),
        ],
        compiler_params=pltpu.CompilerParams(
            collective_id=2, has_side_effects=True, vmem_limit_bytes=48 << 20
        ),
        name="attend",
    )(length, full, norm_gain.reshape(chunks, width), query_weight, key_weight, value_weight)


def body(
    length,
    residual,
    ssm_input,
    state_in,
    state_out,
    step_raw,
    decay_rate,
    ssm_gain,
    out_weight,
    norm_gain,
    query_weight,
    key_weight,
    value_weight,
):
    normed = ssm_layer(length, ssm_input, state_in, state_out, step_raw, decay_rate, ssm_gain)
    layer_out, full = project(normed, out_weight, residual)
    head_out = attend(length, full, norm_gain, query_weight, key_weight, value_weight)
    return layer_out, head_out


def solution(mesh):
    torus = Mesh(
        mesh.devices.reshape(mesh.shape["doc"], mesh.shape["seq"] // 2, 2, mesh.shape["head"]),
        ("doc", "seq_0", "seq_1", "head"),
    )
    in_specs = (
        P("doc"),
        P(DOC_SEQ, "head"),
        P(DOC_SEQ, "head"),
        P(DOC_SEQ, None),
        P(DOC_SEQ, None),
        P(("doc", "head"), SEQ),
        P("head"),
        P("head"),
        P("head", None),
        P(),
        P(None, "head"),
        P(None, "head"),
        P(None, "head"),
    )
    out_specs = (P(DOC_SEQ, "head"), P(DOC_SEQ, "head"))
    return jax.shard_map(body, mesh=torus, in_specs=in_specs, out_specs=out_specs, check_vma=False)
```
